32 devices in a mesh: pair: 4 (over y, x), side: 2 (over core), blk: 4 (over z).
Axes of the slice: x: 2, y: 2, z: 4, core: 2. Of those that a mesh axis runs over, the one named last changes fastest.
Arguments:
- intersect: float32 [4096, 768], P(('pair', 'side', 'blk')), parts along dimension 0, may hold values from -0.1 to 1.7, as said below
- half_factors: float32 [4096, 384], P(('pair', 'side', 'blk')), parts along dimension 0, may hold values from -0.03 to 1.35, as said below
- z_pattern: int32 [32, 6], P(('pair', 'side', 'blk')), parts along dimension 0, may hold values 0 or 1
Outputs:
- refined_factor: float32 [4096, 768], P(('pair', 'side', 'blk')), parts along dimension 0
The draws below stay inside these ranges and needn't reach their ends.
There are 4 independent parts, one for each index of `pair`. The reference program is written for one: setup_inputs(seed, part) draws one part's arguments, and reference() takes and returns one part's arrays. A program takes and returns all parts, laid end to end along the dimension named above; each array names one. Nothing has to cross between parts.
Inputs may be any that keep to these rules, and one draw needn't show every extreme that they name: As a whole windowed matrix, intersect is symmetric: S[a, b] = S[b, a]. `half_factors`: entries of the other half and outside the grid of blocks are absent or zero. `z_pattern`: 1 keeps a tile of the factor, 0 drops it; diagonal tiles are kept whatever it says.
All inputs are finite; a program needn't handle non-finite values. No bound on the sum of `z_pattern` on one device may be relied on, other than what follows from the above.
Results may differ from the reference program's by a relative error of at most 0.0001.
Values sent between devices are 32-bit elements; how exact they have to be, the bound alone decides.
A program may use at most 64 MiB of HBM per device.

```python
import jax
import jax.numpy as jnp
from jax import lax

TILE = 128
TILES_DEV = 1
ITERS = 2
TILE_ROWS = 8
N_BLK = 4


def diag_values(key):
    rows = TILE * TILES_DEV
    draw_key = jax.random.fold_in(key, 11)
    fraction = jax.random.uniform(draw_key, (2, N_BLK, rows), jnp.float32)
    return 0.7 * jnp.exp(fraction * jnp.log(1.5 / 0.7))


def block_inside(blocks):
    column = jnp.arange(blocks)[:, None] + jnp.arange(3)[None, :] - 1
    return ((column >= 0) & (column < blocks)).astype(jnp.float32)


def window_transpose(field):
    empty = jnp.zeros_like(field[:, :1, :, 0])
    pieces = []
    for slot in range(3):
        source = field[:, :, :, 2 - slot]
        if slot == 2:
            source = jnp.concatenate((source[:, 1:], empty), axis=1)
        if slot == 0:
            source = jnp.concatenate((empty, source[:, :-1]), axis=1)
        pieces.append(jnp.transpose(source, (3, 1, 4, 0, 2)))
    return jnp.stack(pieces, axis=3)


def draw_intersect(key, part):
    rows = TILE * TILES_DEV
    blocks = N_BLK
    shape = (2, blocks, rows, 3, 2, rows)
    sigma = 0.012
    noise_key = jax.random.fold_in(key, 3)
    raw = jnp.clip(jax.random.normal(noise_key, shape, jnp.float32), -6.0, 6.0) * sigma
    tile_key = jax.random.fold_in(key, 5)
    present = jax.random.bernoulli(tile_key, 0.75, (2, blocks, TILES_DEV, 3, 2, TILES_DEV)).astype(jnp.float32)
    present = jnp.repeat(jnp.repeat(present, TILE, axis=2), TILE, axis=5)
    inside = block_inside(blocks)[None, :, None, :, None, None]
    coupling = raw * present * inside
    symmetric = 0.5 * (coupling + window_transpose(coupling))
    eye_side = jnp.eye(2, dtype=jnp.float32)
    eye_rows = jnp.eye(rows, dtype=jnp.float32)
    middle = (jnp.arange(3) == 1).astype(jnp.float32)
    diagonal = diag_values(key)[:, :, :, None, None, None] * eye_side[:, None, None, None, :, None] * eye_rows[None, None, :, None, None, :] * middle[None, None, None, :, None, None]
    return (symmetric + diagonal).reshape(2 * blocks * rows, 6 * rows)


def draw_half_factors(key, part):
    rows = TILE * TILES_DEV
    blocks = N_BLK
    shape = (2, blocks, rows, 3, rows)
    sigma = 0.004
    noise_key = jax.random.fold_in(key, 17)
    raw = jnp.clip(jax.random.normal(noise_key, shape, jnp.float32), -6.0, 6.0) * sigma
    inside = block_inside(blocks)[None, :, None, :, None]
    eye_rows = jnp.eye(rows, dtype=jnp.float32)
    middle = (jnp.arange(3) == 1).astype(jnp.float32)
    scales = 1.0 / jnp.sqrt(diag_values(key))
    diagonal = scales[:, :, :, None, None] * eye_rows[None, None, :, None, :] * middle[None, None, None, :, None]
    return (raw * inside + diagonal).reshape(2 * blocks * rows, 3 * rows)


def set_ends(array, rng, low, top_value):
    index_at = [jax.random.randint(jax.random.fold_in(rng, axis), (), 0, length) for axis, length in enumerate(array.shape)]
    main_axis = array.shape.index(max(array.shape))
    next_to = index_at[:main_axis] + [(index_at[main_axis] + 1) % array.shape[main_axis]] + index_at[main_axis + 1:]
    return array.at[tuple(index_at)].set(low).at[tuple(next_to)].set(top_value)


def setup_inputs(seed: int = 0, part: int = 0) -> dict:
    seeds = jax.random.split(jax.random.key(seed), 4)
    own_keys = jax.random.split(jax.random.fold_in(seeds[3], part), 4)
    return {
        "intersect": draw_intersect(jax.random.fold_in(jax.random.fold_in(seeds[3], part), 71), part),
        "half_factors": draw_half_factors(jax.random.fold_in(jax.random.fold_in(seeds[3], part), 71), part),
        "z_pattern": set_ends((jax.random.randint(own_keys[2], (TILE_ROWS, 6 * TILES_DEV), 0, 4) < 3).astype(jnp.int32), jax.random.fold_in(own_keys[2], 1), 0, 1),
    }


def shift_blocks(field, offset):
    empty = jnp.zeros_like(field[:, :1])
    if offset == 1:
        return jnp.concatenate((field[:, 1:], empty), axis=1)
    if offset == -1:
        return jnp.concatenate((empty, field[:, :-1]), axis=1)
    return field


def shift_slots(term, slot):
    empty = jnp.zeros_like(term[:, :, :, :1])
    if slot == 0:
        return jnp.concatenate((term[:, :, :, 1:], empty), axis=3)
    if slot == 2:
        return jnp.concatenate((empty, term[:, :, :, :2]), axis=3)
    return term


def window_product(left, right):
    total = jnp.zeros_like(right)
    for slot in range(3):
        nearby = shift_blocks(right, slot - 1)
        term = jnp.einsum("sbixk,xbkdyj->sbidyj", left[:, :, :, slot], nearby, precision=lax.Precision.HIGHEST)
        total = total + shift_slots(term, slot)
    return total


def window_cross(factor, image):
    total = jnp.zeros_like(image)
    for slot in range(3):
        near_factor = shift_blocks(factor, slot - 1)
        near_image = shift_blocks(image, slot - 1)
        term = jnp.einsum("xbksi,xbkdyj->sbidyj", near_factor[:, :, :, 2 - slot], near_image, precision=lax.Precision.HIGHEST)
        total = total + shift_slots(term, slot)
    return total


def reference(intersect, half_factors, z_pattern):
    blocks = N_BLK
    rows = intersect.shape[1] // 6
    tiles = z_pattern.shape[1] // 6
    tile = rows // tiles
    intersect_win = intersect.reshape(2, blocks, rows, 3, 2, rows)
    half_win = half_factors.reshape(2, blocks, rows, 3, rows)
    eye_side = jnp.eye(2, dtype=jnp.float32)
    eye_rows = jnp.eye(rows, dtype=jnp.float32)
    middle = (jnp.arange(3) == 1).astype(jnp.float32)
    identity = eye_side[:, None, None, None, :, None] * eye_rows[None, None, :, None, None, :] * middle[None, None, None, :, None, None]
    grid = z_pattern.reshape(2, blocks, tiles, 3, 2, tiles)
    halves = jnp.arange(2)
    tile_ids = jnp.arange(tiles)
    diagonal = (halves[:, None, None, None, None, None] == halves[None, None, None, None, :, None]) & (tile_ids[None, None, :, None, None, None] == tile_ids[None, None, None, None, None, :]) & (jnp.arange(3)[None, None, None, :, None, None] == 1)
    kept = jnp.maximum(grid, diagonal.astype(jnp.int32)).astype(jnp.float32)
    wide = jnp.broadcast_to(kept[:, :, :, None, :, :, :, None], (2, blocks, tiles, tile, 3, 2, tiles, tile))
    keep = wide.reshape(2, blocks, rows, 3, 2, rows)
    factor = half_win[:, :, :, :, None, :] * eye_side[:, None, None, None, :, None]
    for step in range(ITERS):
        image = window_product(intersect_win, factor)
        delta = identity - window_cross(factor, image)
        first = window_product(factor, delta)
        second = window_product(first, delta)
        factor = keep * (factor + 0.5 * first + 0.375 * second)
    return factor.reshape(2 * blocks * rows, 6 * rows)
```

```python
import functools

import jax
import jax.numpy as jnp
from jax import lax
from jax.experimental import pallas as pl
from jax.experimental.pallas import tpu as pltpu
from jax.sharding import PartitionSpec as P

ITERS = 2
MESH = pl.DeviceIdType.MESH
F32 = jnp.float32
BF16 = jnp.bfloat16


def parts(x):
    high = x.astype(BF16)
    return high, (x - high.astype(F32)).astype(BF16)


def mm(a, b, ta=False):
    dims = (((0 if ta else 1,), (0,)), ((), ()))

    def dot(x, y):
        return lax.dot_general(x, y, dims, preferred_element_type=F32)

    cols = b[0].shape[1]
    if cols <= 128:
        wide = dot(a[0], jnp.concatenate(b, axis=1))
        return wide[:, :cols] + wide[:, cols:] + dot(a[1], b[0])
    if ta:
        return dot(a[0], b[0]) + dot(a[1], b[0]) + dot(a[0], b[1])
    rows = a[0].shape[0]
    tall = dot(jnp.concatenate(a, axis=0), b[0])
    return tall[:rows] + tall[rows:] + dot(a[0], b[1])


def put(ref, rows, cols, x):
    high, low = parts(x)
    ref[0, rows, cols] = high
    ref[1, rows, cols] = low


def get(ref, rows, cols):
    return ref[0, rows, cols], ref[1, rows, cols]


def cat(pairs, axis):
    return tuple(jnp.concatenate([p[i] for p in pairs], axis=axis) for i in range(2))


Z_EDGE, Z_S, Z_DIAG, Z_PAT, Z_I, Z_D, Z_F, Z_NEW = 0, 1, 2, 3, 4, 6, 8, 9
Z_COUNT = 10
X_ROW, X_EDGE, X_S, X_DIAG, X_COL, X_DD, X_DN, X_NEWN, X_NEWD, X_NEW = 0, 1, 2, 3, 4, 5, 7, 9, 10, 11
X_COUNT = 12


def kernel(
    n, s_ref, h_ref, p_ref, o_ref,
    sx, hx, edge, edge_x, snb, snb_x, diag, diag_x, pat,
    i_out, d_out, i_in, d_in, d_fw, dcol_out, dcol_in, dn_out, dn_in,
    f_out, f_in, z_out, z_in, zn_out, zn_in, zd_out, zd_in, zd_fw,
    sb, sd, zrow, zcol, znd, dcol, dn, dd,
    zs, zr, xs, xr,
):
    side = lax.axis_index("side")
    c = lax.axis_index("blk")
    R = s_ref.shape[0]
    W = 2 * R
    T = p_ref.shape[0]
    tile = R // T
    has = (c > 0, c < n - 1)
    peer = ({"blk": jnp.maximum(c - 1, 0)}, {"blk": jnp.minimum(c + 1, n - 1)})
    sib = {"side": 1 - side}
    mine = pl.ds(pl.multiple_of(side * R, R), R)
    other = pl.ds(pl.multiple_of((1 - side) * R, R), R)
    full = slice(0, W)
    blk = [slice(e * W, (e + 1) * W) for e in range(3)]
    near = (0, 2)
    sent = []

    def z_copy(m, k, src, buf):
        return pltpu.make_async_remote_copy(
            src_ref=src, dst_ref=buf.at[1 - k], send_sem=zs.at[m, k], recv_sem=zr.at[m, 1 - k],
            device_id=peer[k], device_id_type=MESH)

    def z_send(m, k, src, buf):
        copy = z_copy(m, k, src, buf)
        pl.when(has[k])(copy.start)
        sent.append((has[k], copy))

    def z_wait(m, k, buf):
        copy = pltpu.make_async_remote_copy(
            src_ref=buf.at[k], dst_ref=buf.at[k], send_sem=zs.at[m, k], recv_sem=zr.at[m, k],
            device_id=peer[k], device_id_type=MESH)
        pl.when(has[k])(copy.wait_recv)

    def x_copy(m, k, src, dst):
        return pltpu.make_async_remote_copy(
            src_ref=src, dst_ref=dst, send_sem=xs.at[m, k], recv_sem=xr.at[m, k],
            device_id=sib, device_id_type=MESH)

    def x_send(m, k, src, dst):
        copy = x_copy(m, k, src, dst)
        copy.start()
        sent.append((None, copy))

    def x_wait(m, k, dst):
        x_copy(m, k, dst, dst).wait_recv()

    def forward(m, k, buf, dst):
        copy = x_copy(m, k, buf.at[k], dst.at[k])
        pl.when(has[k])(copy.start)
        sent.append((has[k], copy))

    def forward_wait(m, k, dst):
        pl.when(has[k])(x_copy(m, k, dst.at[k], dst.at[k]).wait_recv)

    barrier = pltpu.get_barrier_semaphore()
    pl.semaphore_signal(barrier, inc=1, device_id=sib, device_id_type=MESH)
    for k in range(2):
        @pl.when(has[k])
        def _():
            pl.semaphore_signal(barrier, inc=1, device_id=peer[k], device_id_type=MESH)

    for k in range(2):
        @pl.when(jnp.logical_not(has[k]))
        def _():
            for ref in (edge, edge_x, snb, snb_x, diag, diag_x, f_in, zd_in, zd_fw, pat):
                ref[k] = jnp.zeros(ref.shape[1:], ref.dtype)
            for ref in (i_in, d_in, d_fw):
                for t in range(ITERS):
                    ref[t, k] = jnp.zeros(ref.shape[2:], ref.dtype)
    zrow[...] = jnp.zeros(zrow.shape, BF16)
    zcol[...] = jnp.zeros(zcol.shape, BF16)
    znd[...] = jnp.zeros(znd.shape, BF16)
    put(sb, mine, slice(None), s_ref[...])
    for e in range(3):
        put(zrow, mine, pl.ds(pl.multiple_of(e * W + side * R, R), R), h_ref[:, e * R:(e + 1) * R])
    pl.semaphore_wait(barrier, 1 + has[0].astype(jnp.int32) + has[1].astype(jnp.int32))

    for k in range(2):
        z_send(Z_EDGE, k, h_ref.at[:, pl.ds(near[k] * R, R)], edge)
    x_send(X_ROW, 0, h_ref, hx)
    x_send(X_ROW, 1, s_ref, sx)
    for k in range(2):
        z_send(Z_S, k, s_ref.at[:, pl.ds(W, W)], snb)
        z_send(Z_PAT, k, p_ref, pat)
    for k in range(2):
        z_send(Z_DIAG, k, h_ref.at[:, pl.ds(R, R)], diag)

    x_wait(X_ROW, 0, hx)
    for e in range(3):
        put(zrow, other, pl.ds(pl.multiple_of(e * W + (1 - side) * R, R), R), hx[:, e * R:(e + 1) * R])
    x_wait(X_ROW, 1, sx)
    put(sb, other, slice(None), sx[...])
    for i in range(2):
        zcol[i, blk[1]] = zrow[i, :, blk[1]]
    for k in range(2):
        z_wait(Z_EDGE, k, edge)
        forward(X_EDGE, k, edge, edge_x)
        rows = pl.ds(pl.multiple_of(near[k] * W + side * R, R), R)
        put(zcol, rows, mine, edge[k])
    for k in range(2):
        z_wait(Z_S, k, snb)
        forward(X_S, k, snb, snb_x)
        put(sd.at[k], mine, full, snb[k])
    for k in range(2):
        forward_wait(X_EDGE, k, edge_x)
        rows = pl.ds(pl.multiple_of(near[k] * W + (1 - side) * R, R), R)
        put(zcol, rows, other, edge_x[k])

    eye = (lax.broadcasted_iota(jnp.int32, (W, R), 0) == lax.broadcasted_iota(jnp.int32, (W, R), 1) + side * R).astype(F32)

    def kept(grid, slot, here):
        rows_out = []
        for a in range(T):
            row = []
            for g in range(2):
                for b in range(T):
                    q = (slot * 2 + g) * T + b
                    value = grid[a:a + 1, q:q + 1].astype(F32)
                    if here and slot == 1 and a == b:
                        value = jnp.maximum(value, (side == g).astype(F32))
                    row.append(jnp.broadcast_to(value, (tile, tile)))
            rows_out.append(jnp.concatenate(row, axis=1))
        return jnp.concatenate(rows_out, axis=0) if T > 1 else rows_out[0]

    def window_of_half(block):
        zero = jnp.zeros_like(block)
        return jnp.concatenate([jnp.where(side == 0, block, zero), jnp.where(side == 0, zero, block)], axis=1)

    old = [window_of_half(h_ref[:, e * R:(e + 1) * R]) for e in range(3)]
    for t in range(ITERS):
        last = t == ITERS - 1
        icc = mm(get(sb, full, slice(None)), get(zcol, slice(None), mine))
        i_out[t] = icc
        for k in range(2):
            z_send(Z_I + t, k, i_out.at[t], i_in.at[t])
        if t == 0:
            for k in range(2):
                forward_wait(X_S, k, snb_x)
                put(sd.at[k], other, full, snb_x[k])
        inear = []
        for k in range(2):
            inear.append(
                mm(get(sb, full, blk[near[k]]), get(zcol, blk[1], mine), ta=True)
                + mm(get(sd.at[k], full, full), get(zcol, blk[near[k]], mine)))
        icc = parts(icc)
        inear = [parts(x) for x in inear]
        icol = cat([inear[0], icc, inear[1]], 0)
        dcc = eye - mm(get(zcol, slice(None), full), icol, ta=True)
        d_out[t] = dcc
        for k in range(2):
            z_send(Z_D + t, k, d_out.at[t], d_in.at[t])
        if t == 0:
            for k in range(2):
                z_wait(Z_DIAG, k, diag)
                forward(X_DIAG, k, diag, diag_x)
                put(znd.at[k], mine, mine, diag[k])
            for k in range(2):
                forward_wait(X_DIAG, k, diag_x)
                put(znd.at[k], other, other, diag_x[k])
        else:
            for k in range(2):
                z_wait(Z_NEW, k, zd_in)
                forward(X_NEWD, k, zd_in, zd_fw)
                put(znd.at[k], mine, full, zd_in[k])
            for k in range(2):
                forward_wait(X_NEWD, k, zd_fw)
                put(znd.at[k], other, full, zd_fw[k])
        dcol_out[t, blk[1]] = dcc
        put(dcol, blk[1], mine, dcc)
        for k in range(2):
            dside = -(mm(get(zrow, full, blk[near[k]]), icc, ta=True) + mm(get(znd.at[k], full, full), inear[k], ta=True))
            dcol_out[t, blk[near[k]]] = dside
            put(dcol, blk[near[k]], mine, dside)
        x_send(X_COL, t, dcol_out.at[t], dcol_in.at[t])
        iside = []
        for k in range(2):
            iside.append(parts(
                mm(get(sb, full, blk[1]), get(zrow, full, pl.ds(pl.multiple_of(near[k] * W + side * R, R), R)))
                + mm(get(sb, full, blk[near[k]]), get(znd.at[k], full, mine))))
        dpart = [mm(get(zrow, full, blk[1]), iside[k], ta=True) for k in range(2)]
        x_wait(X_COL, t, dcol_in.at[t])
        put(dcol, slice(None), other, dcol_in[t])
        fcc = mm(get(zrow, mine, slice(None)), get(dcol, slice(None), full))
        if not last:
            f_out[...] = fcc
            for k in range(2):
                z_send(Z_F, k, f_out, f_in)
            fnear = []
            for k in range(2):
                rows = pl.ds(pl.multiple_of(near[k] * W + side * R, R), R)
                fnear.append(
                    mm(get(zcol, rows, full), get(dcol, blk[1], full))
                    + mm(get(znd.at[k], mine, full), get(dcol, blk[near[k]], full)))
        for k in range(2):
            z_wait(Z_I + t, k, i_in.at[t])
            value = -(dpart[k] + mm(get(zcol, blk[near[k]], full), parts(i_in[t, k]), ta=True))
            dn_out[t, k] = value
            x_send(X_DN + t, k, dn_out.at[t, k], dn_in.at[t, k])
            put(dn.at[k], full, mine, value)
        for k in range(2):
            z_wait(Z_D + t, k, d_in.at[t])
            forward(X_DD + t, k, d_in.at[t], d_fw.at[t])
            put(dd.at[k], full, mine, d_in[t, k])
        for k in range(2):
            x_wait(X_DN + t, k, dn_in.at[t, k])
            put(dn.at[k], full, other, dn_in[t, k])
        for k in range(2):
            forward_wait(X_DD + t, k, d_fw.at[t])
            put(dd.at[k], full, other, d_fw[t, k])
        fside = [
            mm(get(zrow, mine, blk[1]), get(dn.at[k], full, full)) + mm(get(zrow, mine, blk[near[k]]), get(dd.at[k], full, full))
            for k in range(2)
        ]
        fc = parts(fcc)
        fs = [parts(x) for x in fside]
        gcc = mm(cat([fs[0], fc, fs[1]], 1), get(dcol, slice(None), full))
        own = p_ref[...]
        new = [None, None, None]
        new[1] = kept(own, 1, True) * (old[1] + 0.5 * fcc + 0.375 * gcc)
        if not last:
            zd_out[...] = new[1]
            for k in range(2):
                z_send(Z_NEW, k, zd_out, zd_in)
            for k in range(2):
                z_wait(Z_F, k, f_in)
                gnear = mm(parts(fnear[k]), get(dcol, blk[1], full)) + mm(parts(f_in[k]), get(dcol, blk[near[k]], full))
                if True:
                    z_wait(Z_PAT, k, pat)
                    mask = kept(pat.at[k][...], near[1 - k], False)
                zn = mask * (window_of_half(edge[k]) + 0.5 * fnear[k] + 0.375 * gnear)
                zn_out[k] = zn
                x_send(X_NEWN, k, zn_out.at[k], zn_in.at[k])
                rows = pl.ds(pl.multiple_of(near[k] * W + side * R, R), R)
                put(zcol, rows, full, zn)
        for k in range(2):
            e = near[k]
            gside = mm(fc, get(dn.at[k], full, full)) + mm(fs[k], get(dd.at[k], full, full))
            new[e] = kept(own, e, True) * (old[e] + 0.5 * fside[k] + 0.375 * gside)
        if last:
            for e in range(3):
                o_ref[:, blk[e]] = new[e]
        else:
            for e in range(3):
                z_out[:, blk[e]] = new[e]
            x_send(X_NEW, 0, z_out, z_in)
            for e in range(3):
                put(zrow, mine, blk[e], new[e])
            for k in range(2):
                x_wait(X_NEWN, k, zn_in.at[k])
                rows = pl.ds(pl.multiple_of(near[k] * W + (1 - side) * R, R), R)
                put(zcol, rows, full, zn_in[k])
            x_wait(X_NEW, 0, z_in)
            put(zrow, other, slice(None), z_in[...])
            for i in range(2):
                zcol[i, blk[1]] = zrow[i, :, blk[1]]
            old = new

    for cond, copy in sent:
        if cond is None:
            copy.wait_send()
        else:
            pl.when(cond)(copy.wait_send)


def solution(mesh):
    n = mesh.shape["blk"]

    def per_device(intersect, half_factors, z_pattern):
        R = intersect.shape[0]
        W = 2 * R

        def f32(*shape):
            return pltpu.VMEM(shape, F32)

        def b16(*shape):
            return pltpu.VMEM(shape, BF16)

        return pl.pallas_call(
            functools.partial(kernel, n),
            out_shape=jax.ShapeDtypeStruct(intersect.shape, F32),
            in_specs=[pl.BlockSpec(memory_space=pltpu.VMEM)] * 3,
            out_specs=pl.BlockSpec(memory_space=pltpu.VMEM),
            scratch_shapes=[
                f32(R, 3 * W), f32(R, 3 * R), f32(2, R, R), f32(2, R, R), f32(2, R, W), f32(2, R, W),
                f32(2, R, R), f32(2, R, R), pltpu.VMEM((2,) + z_pattern.shape, z_pattern.dtype),
                f32(ITERS, W, R), f32(ITERS, W, R), f32(ITERS, 2, W, R), f32(ITERS, 2, W, R), f32(ITERS, 2, W, R),
                f32(ITERS, 3 * W, R), f32(ITERS, 3 * W, R), f32(ITERS, 2, W, R), f32(ITERS, 2, W, R),
                f32(R, W), f32(2, R, W), f32(R, 3 * W), f32(R, 3 * W), f32(2, R, W), f32(2, R, W),
                f32(R, W), f32(2, R, W), f32(2, R, W),
                b16(2, W, 3 * W), b16(2, 2, W, W), b16(2, W, 3 * W), b16(2, 3 * W, W), b16(2, 2, W, W),
                b16(2, 3 * W, W), b16(2, 2, W, W), b16(2, 2, W, W),
                pltpu.SemaphoreType.DMA((Z_COUNT, 2)), pltpu.SemaphoreType.DMA((Z_COUNT, 2)),
                pltpu.SemaphoreType.DMA((X_COUNT, 2)), pltpu.SemaphoreType.DMA((X_COUNT, 2)),
            ],
            compiler_params=pltpu.CompilerParams(collective_id=0, has_side_effects=True),
        )(intersect, half_factors, z_pattern)

    return jax.shard_map(
        per_device,
        mesh=mesh,
        in_specs=(
            P(("pair", "side", "blk"), None),
            P(("pair", "side", "blk"), None),
            P(("pair", "side", "blk"), None),
        ),
        out_specs=P(("pair", "side", "blk"), None),
        check_vma=False,
    )
```

```python
import functools

import jax
import jax.numpy as jnp
from jax import lax
from jax.experimental import pallas as pl
from jax.experimental.pallas import tpu as pltpu
from jax.sharding import PartitionSpec as P

ITERS = 2
MESH = pl.DeviceIdType.MESH
F32 = jnp.float32
VMEM_KIB = 54200
BF16 = jnp.bfloat16


def parts(x):
    high = x.astype(BF16)
    return high, (x - high.astype(F32)).astype(BF16)


def mm(a, b, ta=False):
    dims = (((0 if ta else 1,), (0,)), ((), ()))

    def dot(x, y):
        return lax.dot_general(x, y, dims, preferred_element_type=F32)

    cols = b[0].shape[1]
    if cols <= 128:
        wide = dot(a[0], jnp.concatenate(b, axis=1))
        return wide[:, :cols] + wide[:, cols:] + dot(a[1], b[0])
    if ta:
        return dot(a[0], b[0]) + dot(a[1], b[0]) + dot(a[0], b[1])
    rows = a[0].shape[0]
    tall = dot(jnp.concatenate(a, axis=0), b[0])
    return tall[:rows] + tall[rows:] + dot(a[0], b[1])


def put(ref, rows, cols, x):
    high, low = parts(x)
    ref[0, rows, cols] = high
    ref[1, rows, cols] = low


def get(ref, rows, cols):
    return ref[0, rows, cols], ref[1, rows, cols]


def cat(pairs, axis):
    return tuple(jnp.concatenate([p[i] for p in pairs], axis=axis) for i in range(2))


def half_of_upper(block):
    split = block.shape[0] // 2
    turned = block.T
    return turned[:split], block[split:]


Z_EDGE, Z_S, Z_DIAG, Z_PAT, Z_I, Z_D, Z_F, Z_NEW = 0, 1, 2, 3, 4, 6, 8, 9
Z_COUNT = 10
X_ROW, X_EDGE, X_S, X_DIAG, X_COL, X_DD, X_DN, X_NEWN, X_NEWD, X_NEW = 0, 1, 2, 3, 4, 5, 7, 9, 10, 11
X_COUNT = 12


def kernel(
    n, s_hbm, h_ref, p_ref, o_ref, k_ref,
    s_ref, s_out,
    sx, hx, edge, edge_x, snb, snb_x, diag, diag_x, pat,
    i_out, d_out, i_in, d_in, d_fw, dcol_out, dcol_in, dn_out, dn_in,
    f_out, f_in, z_out, z_in, zn_out, zn_in, zd_out, zd_in, zd_fw,
    sb, sd, zrow, zcol, znd, dcol, dn, dd,
    zs, zr, xs, xr, ls,
):
    side = lax.axis_index("side")
    c = lax.axis_index("blk")
    R = s_ref.shape[0]
    W = 2 * R
    T = p_ref.shape[0]
    tile = R // T
    has = (c > 0, c < n - 1)
    peer = ({"blk": jnp.maximum(c - 1, 0)}, {"blk": jnp.minimum(c + 1, n - 1)})
    sib = {"side": 1 - side}
    mine = pl.ds(pl.multiple_of(side * R, R), R)
    other = pl.ds(pl.multiple_of((1 - side) * R, R), R)
    full = slice(0, W)
    blk = [slice(e * W, (e + 1) * W) for e in range(3)]
    near = (0, 2)
    sent = []

    def z_copy(m, k, src, buf):
        return pltpu.make_async_remote_copy(
            src_ref=src, dst_ref=buf.at[1 - k], send_sem=zs.at[m, k], recv_sem=zr.at[m, 1 - k],
            device_id=peer[k], device_id_type=MESH)

    def z_send(m, k, src, buf):
        copy = z_copy(m, k, src, buf)
        pl.when(has[k])(copy.start)
        sent.append((has[k], copy))

    def z_wait(m, k, buf):
        copy = pltpu.make_async_remote_copy(
            src_ref=buf.at[k], dst_ref=buf.at[k], send_sem=zs.at[m, k], recv_sem=zr.at[m, k],
            device_id=peer[k], device_id_type=MESH)
        pl.when(has[k])(copy.wait_recv)

    def x_copy(m, k, src, dst):
        return pltpu.make_async_remote_copy(
            src_ref=src, dst_ref=dst, send_sem=xs.at[m, k], recv_sem=xr.at[m, k],
            device_id=sib, device_id_type=MESH)

    def x_send(m, k, src, dst):
        copy = x_copy(m, k, src, dst)
        copy.start()
        sent.append((None, copy))

    def x_wait(m, k, dst):
        x_copy(m, k, dst, dst).wait_recv()

    def forward(m, k, buf, dst):
        copy = x_copy(m, k, buf.at[k], dst.at[k])
        pl.when(has[k])(copy.start)
        sent.append((has[k], copy))

    def forward_wait(m, k, dst):
        pl.when(has[k])(x_copy(m, k, dst.at[k], dst.at[k]).wait_recv)

    barrier = pltpu.get_barrier_semaphore()
    pl.semaphore_signal(barrier, inc=1, device_id=sib, device_id_type=MESH)
    for k in range(2):
        @pl.when(has[k])
        def _():
            pl.semaphore_signal(barrier, inc=1, device_id=peer[k], device_id_type=MESH)

    load = pltpu.make_async_copy(s_hbm, s_ref, ls)
    load.start()
    for k in range(2):
        @pl.when(jnp.logical_not(has[k]))
        def _():
            for ref in (edge, edge_x, snb, snb_x, diag, diag_x, f_in, zd_in, zd_fw, pat):
                ref[k] = jnp.zeros(ref.shape[1:], ref.dtype)
            for ref in (i_in, d_in, d_fw):
                for t in range(ITERS):
                    ref[t, k] = jnp.zeros(ref.shape[2:], ref.dtype)
    zrow[...] = jnp.zeros(zrow.shape, BF16)
    zcol[...] = jnp.zeros(zcol.shape, BF16)
    znd[...] = jnp.zeros(znd.shape, BF16)
    pl.semaphore_wait(barrier, 1 + has[0].astype(jnp.int32) + has[1].astype(jnp.int32))

    for k in range(2):
        z_send(Z_EDGE, k, h_ref.at[:, pl.ds(near[k] * R, R)], edge)
    x_send(X_ROW, 0, h_ref, hx)
    load.wait()
    left, right = s_ref[:, W:W + R], s_ref[:, W + R:2 * W]
    s_out[:R] = jnp.where(side == 0, left, right)
    s_out[R:] = jnp.where(side == 0, right[:R // 2], left.T[R // 2:])
    for k in range(2):
        z_send(Z_S, k, s_out, snb)
        z_send(Z_PAT, k, p_ref, pat)
    x_send(X_ROW, 1, s_ref, sx)
    for k in range(2):
        z_send(Z_DIAG, k, h_ref.at[:, pl.ds(R, R)], diag)

    put(sb, mine, slice(None), s_ref[...])
    for e in range(3):
        put(zrow, mine, pl.ds(pl.multiple_of(e * W + side * R, R), R), h_ref[:, e * R:(e + 1) * R])
    x_wait(X_ROW, 0, hx)
    for e in range(3):
        put(zrow, other, pl.ds(pl.multiple_of(e * W + (1 - side) * R, R), R), hx[:, e * R:(e + 1) * R])
    x_wait(X_ROW, 1, sx)
    put(sb, other, slice(None), sx[...])
    for i in range(2):
        zcol[i, blk[1]] = zrow[i, :, blk[1]]
    for k in range(2):
        z_wait(Z_EDGE, k, edge)
        forward(X_EDGE, k, edge, edge_x)
        rows = pl.ds(pl.multiple_of(near[k] * W + side * R, R), R)
        put(zcol, rows, mine, edge[k])
    for k in range(2):
        z_wait(Z_S, k, snb)
        forward(X_S, k, snb, snb_x)
        put(sd.at[k], mine, mine, snb[k, :R])
    for k in range(2):
        forward_wait(X_EDGE, k, edge_x)
        rows = pl.ds(pl.multiple_of(near[k] * W + (1 - side) * R, R), R)
        put(zcol, rows, other, edge_x[k])

    eye = (lax.broadcasted_iota(jnp.int32, (W, R), 0) == lax.broadcasted_iota(jnp.int32, (W, R), 1) + side * R).astype(F32)

    def kept(grid, slot, here):
        rows_out = []
        for a in range(T):
            row = []
            for g in range(2):
                for b in range(T):
                    q = (slot * 2 + g) * T + b
                    value = grid[a:a + 1, q:q + 1].astype(F32)
                    if here and slot == 1 and a == b:
                        value = jnp.maximum(value, (side == g).astype(F32))
                    row.append(jnp.broadcast_to(value, (tile, tile)))
            rows_out.append(jnp.concatenate(row, axis=1))
        return jnp.concatenate(rows_out, axis=0) if T > 1 else rows_out[0]

    for a in range(T):
        for slot in range(3):
            for g in range(2):
                for b in range(T):
                    q = (slot * 2 + g) * T + b
                    value = p_ref[a:a + 1, q:q + 1].astype(F32)
                    if slot == 1 and a == b:
                        value = jnp.maximum(value, (side == g).astype(F32))
                    k_ref[a * tile:(a + 1) * tile, q * tile:(q + 1) * tile] = jnp.broadcast_to(value, (tile, tile))

    def put_pair(ref, here, there):
        upper = jnp.concatenate([jnp.where(side == 0, here, there), jnp.where(side == 0, there, here)], axis=0)
        put(ref, slice(0, R), slice(R, W), upper)
        put(ref, slice(R, W), slice(0, R), upper.T)

    def window_of_half(block):
        zero = jnp.zeros_like(block)
        return jnp.concatenate([jnp.where(side == 0, block, zero), jnp.where(side == 0, zero, block)], axis=1)

    old = [window_of_half(h_ref[:, e * R:(e + 1) * R]) for e in range(3)]
    for t in range(ITERS):
        last = t == ITERS - 1
        icc = mm(get(sb, full, slice(None)), get(zcol, slice(None), mine))
        i_out[t] = icc
        for k in range(2):
            z_send(Z_I + t, k, i_out.at[t], i_in.at[t])
        if t == 0:
            for k in range(2):
                forward_wait(X_S, k, snb_x)
                put(sd.at[k], other, other, snb_x[k, :R])
                put_pair(sd.at[k], snb[k, R:], snb_x[k, R:])
        inear = []
        for k in range(2):
            inear.append(
                mm(get(sb, full, blk[near[k]]), get(zcol, blk[1], mine), ta=True)
                + mm(get(sd.at[k], full, full), get(zcol, blk[near[k]], mine)))
        icc = parts(icc)
        inear = [parts(x) for x in inear]
        icol = cat([inear[0], icc, inear[1]], 0)
        dcc = eye - mm(get(zcol, slice(None), full), icol, ta=True)
        own_tile = jnp.where(side == 0, dcc[:R], dcc[R:])
        off_tile = jnp.where(side == 0, dcc[R:], dcc[:R])
        first_half, second_half = half_of_upper(off_tile)
        d_out[t, :R] = own_tile
        d_out[t, R:] = jnp.where(side == 0, first_half, second_half)
        for k in range(2):
            z_send(Z_D + t, k, d_out.at[t], d_in.at[t])
        if t == 0:
            for k in range(2):
                z_wait(Z_DIAG, k, diag)
                forward(X_DIAG, k, diag, diag_x)
                put(znd.at[k], mine, mine, diag[k])
            for k in range(2):
                forward_wait(X_DIAG, k, diag_x)
                put(znd.at[k], other, other, diag_x[k])
        else:
            for k in range(2):
                z_wait(Z_NEW, k, zd_in)
                forward(X_NEWD, k, zd_in, zd_fw)
                put(znd.at[k], mine, full, zd_in[k])
            for k in range(2):
                forward_wait(X_NEWD, k, zd_fw)
                put(znd.at[k], other, full, zd_fw[k])
        dcol_out[t, blk[1]] = dcc
        put(dcol, blk[1], mine, dcc)
        for k in range(2):
            dside = -(mm(get(zrow, full, blk[near[k]]), icc, ta=True) + mm(get(znd.at[k], full, full), inear[k], ta=True))
            dcol_out[t, blk[near[k]]] = dside
            put(dcol, blk[near[k]], mine, dside)
        x_send(X_COL, t, dcol_out.at[t], dcol_in.at[t])
        iside = []
        for k in range(2):
            iside.append(parts(
                mm(get(sb, full, blk[1]), get(zrow, full, pl.ds(pl.multiple_of(near[k] * W + side * R, R), R)))
                + mm(get(sb, full, blk[near[k]]), get(znd.at[k], full, mine))))
        dpart = [mm(get(zrow, full, blk[1]), iside[k], ta=True) for k in range(2)]
        x_wait(X_COL, t, dcol_in.at[t])
        put(dcol, slice(None), other, dcol_in[t])
        fcc = mm(get(zrow, mine, slice(None)), get(dcol, slice(None), full))
        if not last:
            f_out[...] = fcc
            for k in range(2):
                z_send(Z_F, k, f_out, f_in)
            fnear = []
            for k in range(2):
                rows = pl.ds(pl.multiple_of(near[k] * W + side * R, R), R)
                fnear.append(
                    mm(get(zcol, rows, full), get(dcol, blk[1], full))
                    + mm(get(znd.at[k], mine, full), get(dcol, blk[near[k]], full)))
        for k in range(2):
            z_wait(Z_I + t, k, i_in.at[t])
            value = -(dpart[k] + mm(get(zcol, blk[near[k]], full), parts(i_in[t, k]), ta=True))
            dn_out[t, k] = value
            x_send(X_DN + t, k, dn_out.at[t, k], dn_in.at[t, k])
            put(dn.at[k], full, mine, value)
        fc = parts(fcc)
        gcc = mm(fc, get(dcol, blk[1], full))
        fhalf, ghalf = [], []
        for k in range(2):
            x_wait(X_DN + t, k, dn_in.at[t, k])
            put(dn.at[k], full, other, dn_in[t, k])
            fhalf.append(mm(get(zrow, mine, blk[1]), get(dn.at[k], full, full)))
            ghalf.append(mm(fc, get(dn.at[k], full, full)))
        for k in range(2):
            z_wait(Z_D + t, k, d_in.at[t])
            forward(X_DD + t, k, d_in.at[t], d_fw.at[t])
        for k in range(2):
            put(dd.at[k], mine, mine, d_in[t, k, :R])
            forward_wait(X_DD + t, k, d_fw.at[t])
            put(dd.at[k], other, other, d_fw[t, k, :R])
            put_pair(dd.at[k], d_in[t, k, R:], d_fw[t, k, R:])
        fside = [fhalf[k] + mm(get(zrow, mine, blk[near[k]]), get(dd.at[k], full, full)) for k in range(2)]
        fs = [parts(x) for x in fside]
        for k in range(2):
            gcc = gcc + mm(fs[k], get(dcol, blk[near[k]], full))
        own = p_ref[...]
        new = [None, None, None]
        mask = 1.0 if last else kept(own, 1, True)
        new[1] = mask * (old[1] + 0.5 * fcc + 0.375 * gcc)
        if not last:
            zd_out[...] = new[1]
            for k in range(2):
                z_send(Z_NEW, k, zd_out, zd_in)
            for k in range(2):
                z_wait(Z_F, k, f_in)
                gnear = mm(parts(fnear[k]), get(dcol, blk[1], full)) + mm(parts(f_in[k]), get(dcol, blk[near[k]], full))
                if True:
                    z_wait(Z_PAT, k, pat)
                    mask = kept(pat.at[k][...], near[1 - k], False)
                zn = mask * (window_of_half(edge[k]) + 0.5 * fnear[k] + 0.375 * gnear)
                zn_out[k] = zn
                x_send(X_NEWN, k, zn_out.at[k], zn_in.at[k])
                rows = pl.ds(pl.multiple_of(near[k] * W + side * R, R), R)
                put(zcol, rows, full, zn)
        for k in range(2):
            e = near[k]
            gside = ghalf[k] + mm(fs[k], get(dd.at[k], full, full))
            mask = 1.0 if last else kept(own, e, True)
            new[e] = mask * (old[e] + 0.5 * fside[k] + 0.375 * gside)
        if last:
            for e in range(3):
                o_ref[:, blk[e]] = new[e]
        else:
            for e in range(3):
                z_out[:, blk[e]] = new[e]
            x_send(X_NEW, 0, z_out, z_in)
            for e in range(3):
                put(zrow, mine, blk[e], new[e])
            for k in range(2):
                x_wait(X_NEWN, k, zn_in.at[k])
                rows = pl.ds(pl.multiple_of(near[k] * W + (1 - side) * R, R), R)
                put(zcol, rows, full, zn_in[k])
            x_wait(X_NEW, 0, z_in)
            put(zrow, other, slice(None), z_in[...])
            for i in range(2):
                zcol[i, blk[1]] = zrow[i, :, blk[1]]
            old = new

    for cond, copy in sent:
        if cond is None:
            copy.wait_send()
        else:
            pl.when(cond)(copy.wait_send)


def solution(mesh):
    n = mesh.shape["blk"]

    def per_device(intersect, half_factors, z_pattern):
        R = intersect.shape[0]
        W = 2 * R

        def f32(*shape):
            return pltpu.VMEM(shape, F32)

        def b16(*shape):
            return pltpu.VMEM(shape, BF16)

        refined, keep = pl.pallas_call(
            functools.partial(kernel, n),
            out_shape=(jax.ShapeDtypeStruct(intersect.shape, F32), jax.ShapeDtypeStruct(intersect.shape, F32)),
            in_specs=[pl.BlockSpec(memory_space=m) for m in (pltpu.HBM, pltpu.VMEM, pltpu.VMEM)],
            out_specs=[pl.BlockSpec(memory_space=pltpu.VMEM)] * 2,
            scratch_shapes=[
                f32(*intersect.shape), f32(W - R // 2, R),
                f32(R, 3 * W), f32(R, 3 * R), f32(2, R, R), f32(2, R, R), f32(2, W - R // 2, R), f32(2, W - R // 2, R),
                f32(2, R, R), f32(2, R, R), pltpu.VMEM((2,) + z_pattern.shape, z_pattern.dtype),
                f32(ITERS, W, R), f32(ITERS, W - R // 2, R), f32(ITERS, 2, W, R), f32(ITERS, 2, W - R // 2, R), f32(ITERS, 2, W - R // 2, R),
                f32(ITERS, 3 * W, R), f32(ITERS, 3 * W, R), f32(ITERS, 2, W, R), f32(ITERS, 2, W, R),
                f32(R, W), f32(2, R, W), f32(R, 3 * W), f32(R, 3 * W), f32(2, R, W), f32(2, R, W),
                f32(R, W), f32(2, R, W), f32(2, R, W),
                b16(2, W, 3 * W), b16(2, 2, W, W), b16(2, W, 3 * W), b16(2, 3 * W, W), b16(2, 2, W, W),
                b16(2, 3 * W, W), b16(2, 2, W, W), b16(2, 2, W, W),
                pltpu.SemaphoreType.DMA((Z_COUNT, 2)), pltpu.SemaphoreType.DMA((Z_COUNT, 2)),
                pltpu.SemaphoreType.DMA((X_COUNT, 2)), pltpu.SemaphoreType.DMA((X_COUNT, 2)),
                pltpu.SemaphoreType.DMA,
            ],
            compiler_params=pltpu.CompilerParams(collective_id=0, has_side_effects=True, vmem_limit_bytes=VMEM_KIB * 1024),
        )(intersect, half_factors, z_pattern)
        return keep * refined

    return jax.shard_map(
        per_device,
        mesh=mesh,
        in_specs=(
            P(("pair", "side", "blk"), None),
            P(("pair", "side", "blk"), None),
            P(("pair", "side", "blk"), None),
        ),
        out_specs=P(("pair", "side", "blk"), None),
        check_vma=False,
    )
```

```python
import functools

import jax
import jax.numpy as jnp
from jax import lax
from jax.experimental import pallas as pl
from jax.experimental.pallas import tpu as pltpu
from jax.sharding import PartitionSpec as P

ITERS = 2
MESH = pl.DeviceIdType.MESH
F32 = jnp.float32
VMEM_KIB = 54200
BF16 = jnp.bfloat16


def parts(x):
    high = x.astype(BF16)
    return high, (x - high.astype(F32)).astype(BF16)


def mm(a, b, ta=False):
    dims = (((0 if ta else 1,), (0,)), ((), ()))

    def dot(x, y):
        return lax.dot_general(x, y, dims, preferred_element_type=F32)

    cols = b[0].shape[1]
    if cols <= 128:
        wide = dot(a[0], jnp.concatenate(b, axis=1))
        return wide[:, :cols] + wide[:, cols:] + dot(a[1], b[0])
    if ta:
        return dot(a[0], b[0]) + dot(a[1], b[0]) + dot(a[0], b[1])
    rows = a[0].shape[0]
    tall = dot(jnp.concatenate(a, axis=0), b[0])
    return tall[:rows] + tall[rows:] + dot(a[0], b[1])


def put(ref, rows, cols, x):
    high, low = parts(x)
    ref[0, rows, cols] = high
    ref[1, rows, cols] = low


def get(ref, rows, cols):
    return ref[0, rows, cols], ref[1, rows, cols]


def cat(pairs, axis):
    return tuple(jnp.concatenate([p[i] for p in pairs], axis=axis) for i in range(2))


def half_of_upper(block):
    split = block.shape[0] // 2
    turned = block.T
    return turned[:split], block[split:]


Z_EDGE, Z_S, Z_DIAG, Z_PAT, Z_I, Z_D, Z_F, Z_NEW = 0, 1, 2, 3, 4, 6, 8, 9
Z_COUNT = 10
X_ROW, X_EDGE, X_S, X_DIAG, X_COL, X_DD, X_DN, X_NEWN, X_NEWD, X_NEW = 0, 1, 2, 3, 4, 5, 7, 9, 10, 11
X_COUNT = 12


def kernel(
    n, s_hbm, h_ref, p_ref, o_ref, k_ref,
    s_ref, s_out,
    sx, hx, edge, edge_x, snb, snb_x, diag, diag_x, pat,
    i_out, d_out, i_in, d_in, d_fw, dcol_out, dcol_in, dn_out, dn_in,
    f_out, f_in, z_out, z_in, zn_out, zn_in, zd_out, zd_in, zd_fw,
    sb, sd, zrow, zcol, znd, dcol, dn, dd,
    zs, zr, xs, xr, ls,
):
    side = lax.axis_index("side")
    c = lax.axis_index("blk")
    R = s_ref.shape[0]
    W = 2 * R
    T = p_ref.shape[0]
    tile = R // T
    has = (c > 0, c < n - 1)
    peer = ({"blk": jnp.maximum(c - 1, 0)}, {"blk": jnp.minimum(c + 1, n - 1)})
    sib = {"side": 1 - side}
    mine = pl.ds(pl.multiple_of(side * R, R), R)
    other = pl.ds(pl.multiple_of((1 - side) * R, R), R)
    full = slice(0, W)
    blk = [slice(e * W, (e + 1) * W) for e in range(3)]
    near = (0, 2)
    sent = []

    def z_copy(m, k, src, buf):
        return pltpu.make_async_remote_copy(
            src_ref=src, dst_ref=buf.at[1 - k], send_sem=zs.at[m, k], recv_sem=zr.at[m, 1 - k],
            device_id=peer[k], device_id_type=MESH)

    def z_send(m, k, src, buf):
        copy = z_copy(m, k, src, buf)
        pl.when(has[k])(copy.start)
        sent.append((has[k], copy))

    def z_wait(m, k, buf):
        copy = pltpu.make_async_remote_copy(
            src_ref=buf.at[k], dst_ref=buf.at[k], send_sem=zs.at[m, k], recv_sem=zr.at[m, k],
            device_id=peer[k], device_id_type=MESH)
        pl.when(has[k])(copy.wait_recv)

    def x_copy(m, k, src, dst):
        return pltpu.make_async_remote_copy(
            src_ref=src, dst_ref=dst, send_sem=xs.at[m, k], recv_sem=xr.at[m, k],
            device_id=sib, device_id_type=MESH)

    def x_send(m, k, src, dst):
        copy = x_copy(m, k, src, dst)
        copy.start()
        sent.append((None, copy))

    def x_wait(m, k, dst):
        x_copy(m, k, dst, dst).wait_recv()

    def forward(m, k, buf, dst):
        copy = x_copy(m, k, buf.at[k], dst.at[k])
        pl.when(has[k])(copy.start)
        sent.append((has[k], copy))

    def forward_wait(m, k, dst):
        pl.when(has[k])(x_copy(m, k, dst.at[k], dst.at[k]).wait_recv)

    barrier = pltpu.get_barrier_semaphore()
    pl.semaphore_signal(barrier, inc=1, device_id=sib, device_id_type=MESH)
    for k in range(2):
        @pl.when(has[k])
        def _():
            pl.semaphore_signal(barrier, inc=1, device_id=peer[k], device_id_type=MESH)

    load = pltpu.make_async_copy(s_hbm, s_ref, ls)
    load.start()
    for k in range(2):
        @pl.when(jnp.logical_not(has[k]))
        def _():
            for ref in (edge, edge_x, snb, snb_x, diag, diag_x, f_in, zd_in, zd_fw, pat):
                ref[k] = jnp.zeros(ref.shape[1:], ref.dtype)
            for ref in (i_in, d_in, d_fw):
                for t in range(ITERS):
                    ref[t, k] = jnp.zeros(ref.shape[2:], ref.dtype)
    zrow[...] = jnp.zeros(zrow.shape, BF16)
    zcol[...] = jnp.zeros(zcol.shape, BF16)
    znd[...] = jnp.zeros(znd.shape, BF16)
    pl.semaphore_wait(barrier, 1 + has[0].astype(jnp.int32) + has[1].astype(jnp.int32))

    for k in range(2):
        z_send(Z_EDGE, k, h_ref.at[:, pl.ds(near[k] * R, R)], edge)
    x_send(X_ROW, 0, h_ref, hx)
    load.wait()
    left, right = s_ref[:, W:W + R], s_ref[:, W + R:2 * W]
    s_out[:R] = jnp.where(side == 0, left, right)
    s_out[R:] = jnp.where(side == 0, right[:R // 2], left.T[R // 2:])
    for k in range(2):
        z_send(Z_S, k, s_out, snb)
        z_send(Z_PAT, k, p_ref, pat)
    x_send(X_ROW, 1, s_ref, sx)
    for k in range(2):
        z_send(Z_DIAG, k, h_ref.at[:, pl.ds(R, R)], diag)

    put(sb, mine, slice(None), s_ref[...])
    for e in range(3):
        put(zrow, mine, pl.ds(pl.multiple_of(e * W + side * R, R), R), h_ref[:, e * R:(e + 1) * R])
    x_wait(X_ROW, 0, hx)
    for e in range(3):
        put(zrow, other, pl.ds(pl.multiple_of(e * W + (1 - side) * R, R), R), hx[:, e * R:(e + 1) * R])
    x_wait(X_ROW, 1, sx)
    put(sb, other, slice(None), sx[...])
    for i in range(2):
        zcol[i, blk[1]] = zrow[i, :, blk[1]]
    for k in range(2):
        z_wait(Z_EDGE, k, edge)
        forward(X_EDGE, k, edge, edge_x)
        rows = pl.ds(pl.multiple_of(near[k] * W + side * R, R), R)
        put(zcol, rows, mine, edge[k])
    eye = (lax.broadcasted_iota(jnp.int32, (W, R), 0) == lax.broadcasted_iota(jnp.int32, (W, R), 1) + side * R).astype(F32)

    def kept(grid, slot, here):
        rows_out = []
        for a in range(T):
            row = []
            for g in range(2):
                for b in range(T):
                    q = (slot * 2 + g) * T + b
                    value = grid[a:a + 1, q:q + 1].astype(F32)
                    if here and slot == 1 and a == b:
                        value = jnp.maximum(value, (side == g).astype(F32))
                    row.append(jnp.broadcast_to(value, (tile, tile)))
            rows_out.append(jnp.concatenate(row, axis=1))
        return jnp.concatenate(rows_out, axis=0) if T > 1 else rows_out[0]

    for a in range(T):
        for slot in range(3):
            for g in range(2):
                for b in range(T):
                    q = (slot * 2 + g) * T + b
                    value = p_ref[a:a + 1, q:q + 1].astype(F32)
                    if slot == 1 and a == b:
                        value = jnp.maximum(value, (side == g).astype(F32))
                    k_ref[a * tile:(a + 1) * tile, q * tile:(q + 1) * tile] = jnp.broadcast_to(value, (tile, tile))

    def put_pair(ref, here, there):
        upper = jnp.concatenate([jnp.where(side == 0, here, there), jnp.where(side == 0, there, here)], axis=0)
        put(ref, slice(0, R), slice(R, W), upper)
        put(ref, slice(R, W), slice(0, R), upper.T)

    def window_of_half(block):
        zero = jnp.zeros_like(block)
        return jnp.concatenate([jnp.where(side == 0, block, zero), jnp.where(side == 0, zero, block)], axis=1)

    old = [window_of_half(h_ref[:, e * R:(e + 1) * R]) for e in range(3)]
    for t in range(ITERS):
        last = t == ITERS - 1
        icc = mm(get(sb, full, slice(None)), get(zcol, slice(None), mine))
        i_out[t] = icc
        for k in range(2):
            z_send(Z_I + t, k, i_out.at[t], i_in.at[t])
        if t == 0:
            for k in range(2):
                z_wait(Z_S, k, snb)
                forward(X_S, k, snb, snb_x)
                put(sd.at[k], mine, mine, snb[k, :R])
            for k in range(2):
                forward_wait(X_EDGE, k, edge_x)
                rows = pl.ds(pl.multiple_of(near[k] * W + (1 - side) * R, R), R)
                put(zcol, rows, other, edge_x[k])
            for k in range(2):
                forward_wait(X_S, k, snb_x)
                put(sd.at[k], other, other, snb_x[k, :R])
                put_pair(sd.at[k], snb[k, R:], snb_x[k, R:])
        inear = []
        for k in range(2):
            inear.append(
                mm(get(sb, full, blk[near[k]]), get(zcol, blk[1], mine), ta=True)
                + mm(get(sd.at[k], full, full), get(zcol, blk[near[k]], mine)))
        icc = parts(icc)
        inear = [parts(x) for x in inear]
        icol = cat([inear[0], icc, inear[1]], 0)
        dcc = eye - mm(get(zcol, slice(None), full), icol, ta=True)
        own_tile = jnp.where(side == 0, dcc[:R], dcc[R:])
        off_tile = jnp.where(side == 0, dcc[R:], dcc[:R])
        first_half, second_half = half_of_upper(off_tile)
        d_out[t, :R] = own_tile
        d_out[t, R:] = jnp.where(side == 0, first_half, second_half)
        for k in range(2):
            z_send(Z_D + t, k, d_out.at[t], d_in.at[t])
        if t == 0:
            for k in range(2):
                z_wait(Z_DIAG, k, diag)
                forward(X_DIAG, k, diag, diag_x)
                put(znd.at[k], mine, mine, diag[k])
            for k in range(2):
                forward_wait(X_DIAG, k, diag_x)
                put(znd.at[k], other, other, diag_x[k])
        else:
            for k in range(2):
                z_wait(Z_NEW, k, zd_in)
                forward(X_NEWD, k, zd_in, zd_fw)
                put(znd.at[k], mine, full, zd_in[k])
            for k in range(2):
                forward_wait(X_NEWD, k, zd_fw)
                put(znd.at[k], other, full, zd_fw[k])
        dcol_out[t, blk[1]] = dcc
        put(dcol, blk[1], mine, dcc)
        for k in range(2):
            dside = -(mm(get(zrow, full, blk[near[k]]), icc, ta=True) + mm(get(znd.at[k], full, full), inear[k], ta=True))
            dcol_out[t, blk[near[k]]] = dside
            put(dcol, blk[near[k]], mine, dside)
        x_send(X_COL, t, dcol_out.at[t], dcol_in.at[t])
        iside = []
        for k in range(2):
            iside.append(parts(
                mm(get(sb, full, blk[1]), get(zrow, full, pl.ds(pl.multiple_of(near[k] * W + side * R, R), R)))
                + mm(get(sb, full, blk[near[k]]), get(znd.at[k], full, mine))))
        dpart = [mm(get(zrow, full, blk[1]), iside[k], ta=True) for k in range(2)]
        x_wait(X_COL, t, dcol_in.at[t])
        put(dcol, slice(None), other, dcol_in[t])
        fcc = mm(get(zrow, mine, slice(None)), get(dcol, slice(None), full))
        if not last:
            f_out[...] = fcc
            for k in range(2):
                z_send(Z_F, k, f_out, f_in)
            fnear = []
            for k in range(2):
                rows = pl.ds(pl.multiple_of(near[k] * W + side * R, R), R)
                fnear.append(
                    mm(get(zcol, rows, full), get(dcol, blk[1], full))
                    + mm(get(znd.at[k], mine, full), get(dcol, blk[near[k]], full)))
        for k in range(2):
            z_wait(Z_I + t, k, i_in.at[t])
            value = -(dpart[k] + mm(get(zcol, blk[near[k]], full), parts(i_in[t, k]), ta=True))
            dn_out[t, k] = value
            x_send(X_DN + t, k, dn_out.at[t, k], dn_in.at[t, k])
            put(dn.at[k], full, mine, value)
        fc = parts(fcc)
        gcc = mm(fc, get(dcol, blk[1], full))
        fhalf, ghalf = [], []
        for k in range(2):
            x_wait(X_DN + t, k, dn_in.at[t, k])
            put(dn.at[k], full, other, dn_in[t, k])
            fhalf.append(mm(get(zrow, mine, blk[1]), get(dn.at[k], full, full)))
            ghalf.append(mm(fc, get(dn.at[k], full, full)))
        for k in range(2):
            z_wait(Z_D + t, k, d_in.at[t])
            forward(X_DD + t, k, d_in.at[t], d_fw.at[t])
        for k in range(2):
            put(dd.at[k], mine, mine, d_in[t, k, :R])
            forward_wait(X_DD + t, k, d_fw.at[t])
            put(dd.at[k], other, other, d_fw[t, k, :R])
            put_pair(dd.at[k], d_in[t, k, R:], d_fw[t, k, R:])
        fside = [fhalf[k] + mm(get(zrow, mine, blk[near[k]]), get(dd.at[k], full, full)) for k in range(2)]
        fs = [parts(x) for x in fside]
        for k in range(2):
            gcc = gcc + mm(fs[k], get(dcol, blk[near[k]], full))
        own = p_ref[...]
        new = [None, None, None]
        mask = 1.0 if last else kept(own, 1, True)
        new[1] = mask * (old[1] + 0.5 * fcc + 0.375 * gcc)
        if not last:
            zd_out[...] = new[1]
            for k in range(2):
                z_send(Z_NEW, k, zd_out, zd_in)
            for k in range(2):
                z_wait(Z_F, k, f_in)
                gnear = mm(parts(fnear[k]), get(dcol, blk[1], full)) + mm(parts(f_in[k]), get(dcol, blk[near[k]], full))
                if True:
                    z_wait(Z_PAT, k, pat)
                    mask = kept(pat.at[k][...], near[1 - k], False)
                zn = mask * (window_of_half(edge[k]) + 0.5 * fnear[k] + 0.375 * gnear)
                zn_out[k] = zn
                x_send(X_NEWN, k, zn_out.at[k], zn_in.at[k])
                rows = pl.ds(pl.multiple_of(near[k] * W + side * R, R), R)
                put(zcol, rows, full, zn)
        for k in range(2):
            e = near[k]
            gside = ghalf[k] + mm(fs[k], get(dd.at[k], full, full))
            mask = 1.0 if last else kept(own, e, True)
            new[e] = mask * (old[e] + 0.5 * fside[k] + 0.375 * gside)
        if last:
            for e in range(3):
                o_ref[:, blk[e]] = new[e]
        else:
            for e in range(3):
                z_out[:, blk[e]] = new[e]
            x_send(X_NEW, 0, z_out, z_in)
            for e in range(3):
                put(zrow, mine, blk[e], new[e])
            for k in range(2):
                x_wait(X_NEWN, k, zn_in.at[k])
                rows = pl.ds(pl.multiple_of(near[k] * W + (1 - side) * R, R), R)
                put(zcol, rows, full, zn_in[k])
            x_wait(X_NEW, 0, z_in)
            put(zrow, other, slice(None), z_in[...])
            for i in range(2):
                zcol[i, blk[1]] = zrow[i, :, blk[1]]
            old = new

    for cond, copy in sent:
        if cond is None:
            copy.wait_send()
        else:
            pl.when(cond)(copy.wait_send)


def solution(mesh):
    n = mesh.shape["blk"]

    def per_device(intersect, half_factors, z_pattern):
        R = intersect.shape[0]
        W = 2 * R

        def f32(*shape):
            return pltpu.VMEM(shape, F32)

        def b16(*shape):
            return pltpu.VMEM(shape, BF16)

        refined, keep = pl.pallas_call(
            functools.partial(kernel, n),
            out_shape=(jax.ShapeDtypeStruct(intersect.shape, F32), jax.ShapeDtypeStruct(intersect.shape, F32)),
            in_specs=[pl.BlockSpec(memory_space=m) for m in (pltpu.HBM, pltpu.VMEM, pltpu.VMEM)],
            out_specs=[pl.BlockSpec(memory_space=pltpu.VMEM)] * 2,
            scratch_shapes=[
                f32(*intersect.shape), f32(W - R // 2, R),
                f32(R, 3 * W), f32(R, 3 * R), f32(2, R, R), f32(2, R, R), f32(2, W - R // 2, R), f32(2, W - R // 2, R),
                f32(2, R, R), f32(2, R, R), pltpu.VMEM((2,) + z_pattern.shape, z_pattern.dtype),
                f32(ITERS, W, R), f32(ITERS, W - R // 2, R), f32(ITERS, 2, W, R), f32(ITERS, 2, W - R // 2, R), f32(ITERS, 2, W - R // 2, R),
                f32(ITERS, 3 * W, R), f32(ITERS, 3 * W, R), f32(ITERS, 2, W, R), f32(ITERS, 2, W, R),
                f32(R, W), f32(2, R, W), f32(R, 3 * W), f32(R, 3 * W), f32(2, R, W), f32(2, R, W),
                f32(R, W), f32(2, R, W), f32(2, R, W),
                b16(2, W, 3 * W), b16(2, 2, W, W), b16(2, W, 3 * W), b16(2, 3 * W, W), b16(2, 2, W, W),
                b16(2, 3 * W, W), b16(2, 2, W, W), b16(2, 2, W, W),
                pltpu.SemaphoreType.DMA((Z_COUNT, 2)), pltpu.SemaphoreType.DMA((Z_COUNT, 2)),
                pltpu.SemaphoreType.DMA((X_COUNT, 2)), pltpu.SemaphoreType.DMA((X_COUNT, 2)),
                pltpu.SemaphoreType.DMA,
            ],
            compiler_params=pltpu.CompilerParams(collective_id=0, has_side_effects=True, vmem_limit_bytes=VMEM_KIB * 1024),
        )(intersect, half_factors, z_pattern)
        return keep * refined

    return jax.shard_map(
        per_device,
        mesh=mesh,
        in_specs=(
            P(("pair", "side", "blk"), None),
            P(("pair", "side", "blk"), None),
            P(("pair", "side", "blk"), None),
        ),
        out_specs=P(("pair", "side", "blk"), None),
        check_vma=False,
    )
```
